128 devices in a mesh: layer: 8 (over x_lo, z), feat: 16 (over y, x_hi, core).
Axes of the slice: x: 4 (x_hi: 2, x_lo: 2; x = x_hi * 2 + x_lo), y: 4, z: 4, core: 2. Of those that a mesh axis runs over, the one named last changes fastest.
Arguments:
- sources: bfloat16 [8, 1024, 2304], P('layer', 'feat'), may hold values from -6 to 6
- w_encode: bfloat16 [8, 2304, 16384], P('layer', None, 'feat'), may hold values from -0.125 to 0.125
- b_encode: float32 [8, 16384], P('layer', 'feat'), may hold values from -3 to 3
- w_decode: bfloat16 [8, 16384, 2304], P('layer', 'feat'), may hold values from -0.046875 to 0.046875
- b_decode: float32 [2304], replicated, may hold values from -3 to 3
- target: bfloat16 [1024, 2304], replicated, may hold values from -6 to 6
Outputs:
- error: float32 [1024, 2304], P(('layer', 'feat'))
- feature_grad: bfloat16 [8, 1024, 16384], P('layer', None, 'feat')
- decoder_grad: bfloat16 [8, 16384, 2304], P('layer', 'feat')
The draws below stay inside these ranges and needn't reach their ends.
All inputs are finite; a program needn't handle non-finite values.
Results may differ from the reference program's by a relative error of at most 0.0056.
Values may be sent and summed in bfloat16 or wider, within the bound.
No kernel may reach another device: no remote copies, remote signals or barrier semaphores. Data moves between devices by JAX's collectives and lax.ppermute only.
A program may use at most 128 MiB of HBM per device.

```python
import math
import jax
import jax.numpy as jnp
from jax import lax

D = 2304
F = 16384
TOKENS = 1024
LAYERS = 8


def block_scale(stream_key, dims, shards, smallest, high):
    factor_of, own = 1.0, jax.random.fold_in(stream_key, 6)
    for position, parts in shards:
        steps = jnp.exp(jax.random.uniform(jax.random.fold_in(own, position), (parts,), jnp.float32, smallest / len(shards), high / len(shards)))
        factor_of = factor_of * jnp.repeat(steps, dims[position] // parts).reshape([-1 if axis == position else 1 for axis in range(len(dims))])
    return factor_of


def noise(rng, dims, scale, most, pieces=(), held_as=jnp.bfloat16):
    drawn = scale * jax.random.normal(rng, dims, jnp.float32)
    if pieces:
        drawn = drawn * block_scale(rng, dims, pieces, -0.22, 0.18)
    return jnp.clip(drawn, -most, most).astype(held_as)


def setup_inputs(seed: int = 0) -> dict:
    seeds = jax.random.split(jax.random.key(seed), 7)
    sources = noise(seeds[0], (LAYERS, TOKENS, D), 1.0, 6.0, ((0, 8), (1, 16)))
    w_encode = noise(seeds[1], (LAYERS, D, F), D ** -0.5, 0.125, ((0, 8), (2, 16)))
    b_encode = noise(seeds[2], (LAYERS, F), 0.5, 3.0, ((0, 8), (1, 16)), jnp.float32)
    w_decode = noise(seeds[3], (LAYERS, F, D), F ** -0.5, 0.046875, ((0, 8), (1, 16)))
    b_decode = noise(seeds[4], (D,), 0.5, 3.0, (), jnp.float32)
    target = noise(seeds[5], (TOKENS, D), 1.0, 6.0)
    return {"sources": sources, "w_encode": w_encode, "b_encode": b_encode, "w_decode": w_decode, "b_decode": b_decode, "target": target}


def reference(sources, w_encode, b_encode, w_decode, b_decode, target):
    scale = 1.0 / math.sqrt(TOKENS)
    recon = jnp.zeros((TOKENS, D), jnp.float32)
    acts_list = []
    for layer_index in range(LAYERS):
        pre = jnp.dot(sources[layer_index], w_encode[layer_index], preferred_element_type=jnp.float32) + b_encode[layer_index]
        acts = jnp.maximum(pre, 0.0).astype(jnp.bfloat16)
        acts_list.append(acts)
        recon = recon + jnp.dot(acts, w_decode[layer_index], preferred_element_type=jnp.float32)
    error = recon + b_decode - target.astype(jnp.float32)
    error_low = error.astype(jnp.bfloat16)
    feature_list = []
    decoder_list = []
    for layer_index in range(LAYERS):
        grad_feat = lax.dot_general(error_low, w_decode[layer_index], (((1,), (1,)), ((), ())), preferred_element_type=jnp.float32)
        feature_list.append(grad_feat.astype(jnp.bfloat16))
        grad_dec = lax.dot_general(acts_list[layer_index], error_low, (((0,), (0,)), ((), ())), preferred_element_type=jnp.float32)
        decoder_list.append((grad_dec * scale).astype(jnp.bfloat16))
    return (error, jnp.stack(feature_list), jnp.stack(decoder_list))
```

```python
import math

import jax
import jax.numpy as jnp
from jax import lax
from jax.experimental import pallas as pl
from jax.experimental.pallas import tpu as pltpu
from jax.sharding import Mesh
from jax.sharding import PartitionSpec as P


AXES = ("xl", "z", "y", "xh", "c")
LAYER = ("xl", "z")
FEAT = ("y", "xh", "c")
DEVICES = [
    (xl, z, y, xh, c)
    for xl in range(2)
    for z in range(4)
    for y in range(4)
    for xh in range(2)
    for c in range(2)
]


def index(xl, z, y, xh, c):
    return (((xl * 4 + z) * 4 + y) * 2 + xh) * 2 + c


def pairs(to):
    return [(index(*d), index(*to(*d))) for d in DEVICES]


def move(value, to):
    return lax.ppermute(value, AXES, pairs(to))


def by_y(k):
    return lambda xl, z, y, xh, c: (xl, z, y ^ k, xh, c)


def by_x(k):
    return lambda xl, z, y, xh, c: (xl ^ (k & 1), z, y, xh ^ (k >> 1), c)


def by_z(k):
    return lambda xl, z, y, xh, c: (xl, z ^ k, y, xh, c)


def by_xh(xl, z, y, xh, c):
    return (xl, z, y, xh ^ 1, c)


def by_core(xl, z, y, xh, c):
    return (xl, z, y, xh, c ^ 1)


def first(k):
    return lambda xl, z, y, xh, c: (by_y(k) if c == 0 else by_x(k))(xl, z, y, xh, c)


def second(k):
    return lambda xl, z, y, xh, c: (by_x(k) if c == 0 else by_y(k))(xl, z, y, xh, c)


def owner(xl, z, y, xh, c):
    return (y >> 1, ((y & 1) << 1) | xh, (c << 1) | xl, z >> 1, z & 1)


def params(*semantics):
    return pltpu.CompilerParams(dimension_semantics=semantics)


def whole(shape):
    return pl.BlockSpec(shape, lambda j: (0,) * len(shape))


def encode(pieces, weight, bias):
    rows, depth = pieces[0].shape
    width = weight.shape[1]
    tile = 256
    total = rows * len(pieces)

    def kernel(*refs):
        parts, (w_ref, b_ref, out_ref, x_ref) = refs[: len(pieces)], refs[len(pieces) :]

        @pl.when(pl.program_id(0) == 0)
        def _():
            for i, part in enumerate(parts):
                x_ref[i * rows : (i + 1) * rows, :] = part[...]

        pre = jnp.dot(x_ref[...], w_ref[...], preferred_element_type=jnp.float32) + b_ref[...]
        out_ref[...] = jnp.maximum(pre, 0.0).astype(jnp.bfloat16)

    return pl.pallas_call(
        kernel,
        grid=(width // tile,),
        in_specs=[whole((rows, depth))] * len(pieces)
        + [
            pl.BlockSpec((depth, tile), lambda j: (0, j)),
            pl.BlockSpec((1, tile), lambda j: (0, j)),
        ],
        out_specs=pl.BlockSpec((total, tile), lambda j: (0, j)),
        out_shape=jax.ShapeDtypeStruct((total, width), jnp.bfloat16),
        scratch_shapes=[pltpu.VMEM((total, depth), jnp.bfloat16)],
        compiler_params=params("arbitrary"),
        cost_estimate=pl.CostEstimate(
            flops=2 * total * depth * width,
            bytes_accessed=2 * (total * depth + depth * width + total * width),
            transcendentals=0,
        ),
        name="encode",
    )(*pieces, weight, bias)


def decode(acts, weight):
    rows, feats = acts.shape
    depth = weight.shape[1]
    half = rows // 2
    tile = 768

    def kernel(a_ref, w_ref, keep_ref, send_ref):
        send_ref[...] = jnp.dot(
            a_ref[half:, :], w_ref[...], preferred_element_type=jnp.float32
        ).astype(jnp.bfloat16)
        keep_ref[...] = jnp.dot(a_ref[:half, :], w_ref[...], preferred_element_type=jnp.float32)

    return pl.pallas_call(
        kernel,
        grid=(depth // tile,),
        in_specs=[whole((rows, feats)), pl.BlockSpec((feats, tile), lambda j: (0, j))],
        out_specs=[pl.BlockSpec((half, tile), lambda j: (0, j))] * 2,
        out_shape=[
            jax.ShapeDtypeStruct((half, depth), jnp.float32),
            jax.ShapeDtypeStruct((half, depth), jnp.bfloat16),
        ],
        compiler_params=params("arbitrary"),
        cost_estimate=pl.CostEstimate(
            flops=2 * rows * feats * depth,
            bytes_accessed=2 * (rows * feats + feats * depth) + 6 * half * depth,
            transcendentals=0,
        ),
        name="decode",
    )(acts, weight)


def split_cores(core, keeps, gots):
    depth = keeps[0].shape[1]
    tile = 768
    out_rows = 128

    def kernel(core_ref, k0, k1, g0, g1, own_ref, s1, s2, s3):
        outs = (own_ref, s1, s2, s3)
        keep, got = (k0, k1), (g0, g1)
        for flip in range(2):

            @pl.when(core_ref[0] == flip)
            def _(flip=flip):
                for a in range(4):
                    for b in range(4):
                        dy, dx = (b, a) if flip else (a, b)
                        src = slice((dy * 2 + (dx & 1)) * 32, (dy * 2 + (dx & 1)) * 32 + 32)
                        value = keep[dx >> 1][src, :] + got[dx >> 1][src, :].astype(jnp.float32)
                        outs[a][b * 32 : b * 32 + 32, :] = value.astype(outs[a].dtype)

    block = pl.BlockSpec((256, tile), lambda j: (0, j))
    out_block = pl.BlockSpec((out_rows, tile), lambda j: (0, j))
    return pl.pallas_call(
        kernel,
        grid=(depth // tile,),
        in_specs=[pl.BlockSpec(memory_space=pltpu.SMEM)] + [block] * 4,
        out_specs=[out_block] * 4,
        out_shape=[jax.ShapeDtypeStruct((out_rows, depth), jnp.float32)]
        + [jax.ShapeDtypeStruct((out_rows, depth), jnp.bfloat16)] * 3,
        compiler_params=params("arbitrary"),
        cost_estimate=pl.CostEstimate(flops=0, bytes_accessed=10 * 1024 * 1024, transcendentals=0),
        name="split_cores",
    )(core, *keeps, *gots)


def split_first(own, gots):
    rows, depth = own.shape
    part = rows // 4
    tile = 768

    def kernel(own_ref, g1, g2, g3, keep_ref, s1, s2, s3):
        for b, out in enumerate((keep_ref, s1, s2, s3)):
            src = slice(b * part, (b + 1) * part)
            value = own_ref[src, :]
            for got in (g1, g2, g3):
                value = value + got[src, :].astype(jnp.float32)
            out[...] = value.astype(out.dtype)

    block = pl.BlockSpec((rows, tile), lambda j: (0, j))
    out_block = pl.BlockSpec((part, tile), lambda j: (0, j))
    return pl.pallas_call(
        kernel,
        grid=(depth // tile,),
        in_specs=[block] * 4,
        out_specs=[out_block] * 4,
        out_shape=[jax.ShapeDtypeStruct((part, depth), jnp.float32)]
        + [jax.ShapeDtypeStruct((part, depth), jnp.bfloat16)] * 3,
        compiler_params=params("arbitrary"),
        cost_estimate=pl.CostEstimate(flops=0, bytes_accessed=4 * 1024 * 1024, transcendentals=0),
        name="split_first",
    )(own, *gots)


def gradients(place, mine, theirs, acts, decoder, scale):
    feats, depth = decoder.shape
    tokens = 1024
    tile = 256

    def kernel(place_ref, *refs):
        parts, (a0, a1, w_ref, fg_ref, dg_ref, e_ref, x_ref) = refs[:8], refs[8:]
        y, xh, c, xl = (place_ref[i] for i in range(4))

        def row(dy, dh, dc, dxl):
            where = ((((y ^ dy) * 2 + (xh ^ dh)) * 2 + (c ^ dc)) * 2 + (xl ^ dxl)) * 32
            return pl.ds(pl.multiple_of(where, 32), 32)

        @pl.when(pl.program_id(0) == 0)
        def _():
            for flip in range(2):

                @pl.when(c == flip)
                def _(flip=flip):
                    for dc in range(2):
                        for a in range(4):
                            for b in range(4):
                                dy, dx = (b, a) if flip ^ dc else (a, b)
                                e_ref[row(dy, dx >> 1, dc, dx & 1), :] = parts[dc * 4 + a][
                                    b * 32 : b * 32 + 32, :
                                ]

        for dh, act in enumerate((a0, a1)):
            for dc in range(2):
                for dy in range(4):
                    for dxl in range(2):
                        src = ((dc * 4 + dy) * 2 + dxl) * 32
                        x_ref[row(dy, dh, dc, dxl), :] = act[src : src + 32, :]
        error = e_ref[...]
        fg_ref[...] = lax.dot_general(
            error, w_ref[...], (((1,), (1,)), ((), ())), preferred_element_type=jnp.float32
        ).astype(jnp.bfloat16)
        dg_ref[...] = (
            lax.dot_general(
                x_ref[...], error, (((0,), (0,)), ((), ())), preferred_element_type=jnp.float32
            )
            * scale
        ).astype(jnp.bfloat16)

    return pl.pallas_call(
        kernel,
        grid=(feats // tile,),
        in_specs=[pl.BlockSpec(memory_space=pltpu.SMEM)]
        + [whole((128, depth))] * 8
        + [pl.BlockSpec((512, tile), lambda j: (0, j))] * 2
        + [pl.BlockSpec((tile, depth), lambda j: (j, 0))],
        out_specs=[
            pl.BlockSpec((tokens, tile), lambda j: (0, j)),
            pl.BlockSpec((tile, depth), lambda j: (j, 0)),
        ],
        out_shape=[
            jax.ShapeDtypeStruct((tokens, feats), jnp.bfloat16),
            jax.ShapeDtypeStruct((feats, depth), jnp.bfloat16),
        ],
        scratch_shapes=[
            pltpu.VMEM((tokens, depth), jnp.bfloat16),
            pltpu.VMEM((tokens, tile), jnp.bfloat16),
        ],
        compiler_params=params("arbitrary"),
        cost_estimate=pl.CostEstimate(
            flops=4 * tokens * feats * depth,
            bytes_accessed=2 * (tokens * depth + 2 * feats * depth + 2 * tokens * feats),
            transcendentals=0,
        ),
        name="gradients",
    )(place, *mine, *theirs, *acts, decoder)


def body(sources, w_encode, b_encode, w_decode, b_decode, target):
    encoder, decoder = w_encode[0], w_decode[0]
    xl, z, y, xh, c = (lax.axis_index(name) for name in AXES)
    scale = 1.0 / math.sqrt(target.shape[0])

    block = sources[0]
    block = jnp.where(xl == 0, block, jnp.concatenate([block[32:], block[:32]], axis=0))
    across = move(block, by_xh)
    near = [block] + [move(block, by_y(k)) for k in (1, 2, 3)]
    far = [across, move(across, by_y(1)), move(near[2], by_xh), move(across, by_y(3))]
    acts, keeps, gots = [], [], []
    for group in (near, far):
        pieces = group + [move(piece, by_core) for piece in group]
        acts.append(encode(pieces, encoder, b_encode))
        keep, send = decode(acts[-1], decoder)
        keeps.append(keep)
        gots.append(move(send, by_core))

    core = c.astype(jnp.int32).reshape(1)
    own, *sends = split_cores(core, keeps, gots)
    gots = [move(send, first(k + 1)) for k, send in enumerate(sends)]
    own, *sends = split_first(own, gots)
    gots = [move(send, second(k + 1)) for k, send in enumerate(sends)]
    own = own + sum(got.astype(jnp.float32) for got in gots)
    send = own.astype(jnp.bfloat16)
    gots = [move(send, by_z(k)) for k in (1, 2, 3)]
    own = own + sum(got.astype(jnp.float32) for got in gots)

    granule = ((y * 2 + xh) * 2 + c) * 2 + xl
    error = own + b_decode - lax.dynamic_slice_in_dim(target, granule * 32, 32, 0).astype(jnp.float32)
    low = error.astype(jnp.bfloat16)
    error_out = move(lax.dynamic_slice_in_dim(error, z * 8, 8, 0), owner)

    low = jnp.concatenate([low] + [move(low, second(k)) for k in (1, 2, 3)], axis=0)
    mine = [low] + [move(low, first(k)) for k in (1, 2, 3)]
    theirs = [move(piece, by_core) for piece in mine]
    place = jnp.stack([y, xh, c, xl]).astype(jnp.int32)
    feature_grad, decoder_grad = gradients(place, mine, theirs, acts, decoder, scale)
    return error_out, feature_grad[None], decoder_grad[None]


def solution(mesh):
    grid = Mesh(mesh.devices.reshape(2, 4, 4, 2, 2), AXES)
    return jax.shard_map(
        body,
        mesh=grid,
        in_specs=(
            P(LAYER, FEAT, None),
            P(LAYER, None, FEAT),
            P(LAYER, FEAT),
            P(LAYER, FEAT, None),
            P(),
            P(),
        ),
        out_specs=(P(AXES, None), P(LAYER, None, FEAT), P(LAYER, FEAT, None)),
        check_vma=False,
    )
```

```python
import math

import jax
import jax.numpy as jnp
from jax import lax
from jax.experimental import pallas as pl
from jax.experimental.pallas import tpu as pltpu
from jax.sharding import Mesh
from jax.sharding import PartitionSpec as P


AXES = ("xl", "z", "y", "xh", "c")
LAYER = ("xl", "z")
FEAT = ("y", "xh", "c")
DEVICES = [
    (xl, z, y, xh, c)
    for xl in range(2)
    for z in range(4)
    for y in range(4)
    for xh in range(2)
    for c in range(2)
]


def index(xl, z, y, xh, c):
    return (((xl * 4 + z) * 4 + y) * 2 + xh) * 2 + c


def pairs(to):
    return [(index(*d), index(*to(*d))) for d in DEVICES]


def move(value, to):
    return lax.ppermute(value, AXES, pairs(to))


def by_y(k):
    return lambda xl, z, y, xh, c: (xl, z, y ^ k, xh, c)


def by_x(k):
    return lambda xl, z, y, xh, c: (xl ^ (k & 1), z, y, xh ^ (k >> 1), c)


def by_z(k):
    return lambda xl, z, y, xh, c: (xl, z ^ k, y, xh, c)


def by_xh(xl, z, y, xh, c):
    return (xl, z, y, xh ^ 1, c)


def by_core(xl, z, y, xh, c):
    return (xl, z, y, xh, c ^ 1)


def first(k):
    return lambda xl, z, y, xh, c: (by_y(k) if c == 0 else by_x(k))(xl, z, y, xh, c)


def second(k):
    return lambda xl, z, y, xh, c: (by_x(k) if c == 0 else by_y(k))(xl, z, y, xh, c)


def owner(xl, z, y, xh, c):
    return (y >> 1, ((y & 1) << 1) | xh, (c << 1) | xl, z >> 1, z & 1)


SPANS = ((0, 1280), (1280, 2304))
MIB = 1024 * 1024
VMEM = pl.BlockSpec(memory_space=pltpu.VMEM)
HBM = pl.BlockSpec(memory_space=pltpu.HBM)


def call(kernel, args, outs, *, limit, flops=0, moved=0, specs=None, scratch=()):
    return pl.pallas_call(
        kernel,
        in_specs=specs or [VMEM] * len(args),
        out_specs=[VMEM] * len(outs),
        out_shape=[jax.ShapeDtypeStruct(shape, dtype) for shape, dtype in outs],
        scratch_shapes=list(scratch),
        compiler_params=pltpu.CompilerParams(vmem_limit_bytes=limit * MIB),
        cost_estimate=pl.CostEstimate(
            flops=int(flops), bytes_accessed=int(moved), transcendentals=0
        ),
    )(*args)


def prefetch(*arrays):
    def kernel(*refs):
        count = len(arrays)
        ins, outs, sems = refs[:count], refs[count : 2 * count], refs[2 * count]
        copies = [pltpu.make_async_copy(ins[i], outs[i], sems.at[i]) for i in range(count)]
        for copy in copies:
            copy.start()
        for copy in copies:
            copy.wait()

    return call(
        kernel,
        arrays,
        [(a.shape, a.dtype) for a in arrays],
        limit=12,
        moved=sum(a.size * a.dtype.itemsize for a in arrays),
        specs=[HBM] * len(arrays),
        scratch=[pltpu.SemaphoreType.DMA((len(arrays),))],
    )


def encode(pieces, weight, bias):
    rows, depth = pieces[0].shape
    width = weight.shape[1]
    tile = 512
    total = rows * len(pieces)

    def kernel(*refs):
        parts, (w_ref, b_ref, out_ref, x_ref) = refs[: len(pieces)], refs[len(pieces) :]
        for i, part in enumerate(parts):
            x_ref[i * rows : (i + 1) * rows, :] = part[...]
        for j in range(0, width, tile):
            cols = slice(j, j + tile)
            pre = jnp.dot(x_ref[...], w_ref[:, cols], preferred_element_type=jnp.float32)
            out_ref[:, cols] = jnp.maximum(pre + b_ref[:, cols], 0.0).astype(jnp.bfloat16)

    (out,) = call(
        kernel,
        (*pieces, weight, bias),
        [((total, width), jnp.bfloat16)],
        limit=20,
        flops=2 * total * depth * width,
        moved=2 * total * depth,
        scratch=[pltpu.VMEM((total, depth), jnp.bfloat16)],
    )
    return out


def decode(acts, weight, spans):
    rows, feats = acts.shape
    half = rows // 2
    tile = 256

    def kernel(a_ref, w_ref, *outs):
        for i, (begin, end) in enumerate(spans):
            for j in range(begin, end, tile):
                cols = slice(j - begin, j - begin + tile)
                out = jnp.dot(
                    a_ref[...], w_ref[:, j : j + tile], preferred_element_type=jnp.float32
                )
                outs[2 * i][:, cols] = out[:half, :]
                outs[2 * i + 1][:, cols] = out[half:, :].astype(jnp.bfloat16)

    shapes = []
    for begin, end in spans:
        shapes += [((half, end - begin), jnp.float32), ((half, end - begin), jnp.bfloat16)]
    total = sum(end - begin for begin, end in spans)
    return call(
        kernel,
        (acts, weight),
        shapes,
        limit=20,
        flops=2 * rows * feats * total,
        moved=6 * half * total,
    )


def split_cores(keeps, gots):
    width = keeps[0].shape[1]
    rows = 128

    def kernel(k0, k1, g0, g1, *outs):
        keep, got = (k0, k1), (g0, g1)
        core, xl = lax.axis_index("c"), lax.axis_index("xl")
        for flip in range(2):

            @pl.when(core == flip)
            def _(flip=flip):
                for a in range(4):
                    for b in range(4):
                        dy, dx = (b, a) if flip else (a, b)
                        at = pl.multiple_of((dy * 2 + ((dx & 1) ^ xl)) * 32, 32)
                        src = (pl.ds(at, 32), slice(None))
                        value = keep[dx >> 1][src] + got[dx >> 1][src].astype(jnp.float32)
                        outs[a][b * 32 : b * 32 + 32, :] = value.astype(outs[a].dtype)

    return call(
        kernel,
        (*keeps, *gots),
        [((rows, width), jnp.float32)] + [((rows, width), jnp.bfloat16)] * 3,
        limit=12,
        flops=512 * width,
        moved=512 * width * 9,
    )


def split_first(owns, gots):
    rows = owns[0].shape[0]
    part = rows // 4
    depth = SPANS[-1][1]

    def kernel(*refs):
        ins, outs = refs[: 4 * len(SPANS)], refs[4 * len(SPANS) :]
        for i, (begin, end) in enumerate(SPANS):
            own, *others = ins[4 * i : 4 * i + 4]
            for b, out in enumerate(outs):
                src = slice(b * part, (b + 1) * part)
                value = own[src, :]
                for got in others:
                    value = value + got[src, :].astype(jnp.float32)
                out[:, begin:end] = value.astype(out.dtype)

    args = []
    for own, got in zip(owns, gots):
        args += [own, *got]
    return call(
        kernel,
        args,
        [((part, depth), jnp.float32)] + [((part, depth), jnp.bfloat16)] * 3,
        limit=8,
        flops=4 * rows * depth,
        moved=rows * depth * 12,
    )


def add(own, gots):
    def kernel(own_ref, g1, g2, g3, out, low):
        value = own_ref[...]
        for got in (g1, g2, g3):
            value = value + got[...].astype(jnp.float32)
        out[...] = value
        low[...] = value.astype(jnp.bfloat16)

    return call(
        kernel,
        (own, *gots),
        [(own.shape, jnp.float32), (own.shape, jnp.bfloat16)],
        limit=4,
        flops=3 * own.size,
        moved=own.size * 16,
    )


def finish(own, gots, target, bias):
    rows, depth = own.shape

    def kernel(own_ref, g1, g2, g3, t_hbm, b_hbm, rows_ref, low_ref, t_ref, b_ref, err_ref, sems):
        y, xh, c, xl, z = (lax.axis_index(name) for name in ("y", "xh", "c", "xl", "z"))
        at = pl.multiple_of((((y * 2 + xh) * 2 + c) * 2 + xl) * rows, rows)
        one = pltpu.make_async_copy(t_hbm.at[pl.ds(at, rows), :], t_ref, sems.at[0])
        two = pltpu.make_async_copy(b_hbm, b_ref, sems.at[1])
        one.start()
        two.start()
        value = own_ref[...]
        for got in (g1, g2, g3):
            value = value + got[...].astype(jnp.float32)
        one.wait()
        two.wait()
        value = value + b_ref[...] - t_ref[...].astype(jnp.float32)
        err_ref[...] = value
        low_ref[...] = value.astype(jnp.bfloat16)
        rows_ref[...] = err_ref[pl.ds(pl.multiple_of(z * 8, 8), 8), :]

    return call(
        kernel,
        (own, *gots, target, bias),
        [((8, depth), jnp.float32), ((rows, depth), jnp.bfloat16)],
        limit=4,
        flops=6 * own.size,
        moved=own.size * 16,
        specs=[VMEM] * 4 + [HBM] * 2,
        scratch=[
            pltpu.VMEM((rows, depth), jnp.bfloat16),
            pltpu.VMEM((1, depth), jnp.float32),
            pltpu.VMEM((rows, depth), jnp.float32),
            pltpu.SemaphoreType.DMA((2,)),
        ],
    )


def join(pieces):
    rows = pieces[0].shape[0]

    def kernel(*refs):
        ins, outs = refs[: len(pieces)], refs[len(pieces) :]
        for (begin, end), out in zip(SPANS, outs):
            for i, piece in enumerate(ins):
                out[i * rows : (i + 1) * rows, :] = piece[:, begin:end]

    return call(
        kernel,
        pieces,
        [((rows * len(pieces), end - begin), jnp.bfloat16) for begin, end in SPANS],
        limit=4,
        moved=4 * sum(p.size for p in pieces),
    )


def gradients(mine, theirs, acts, decoder, scale, span, partial, made):
    feats, depth = decoder.shape
    begin, end = SPANS[span]
    width = end - begin
    tokens = 1024
    tile = 256
    steps = feats // tile
    last = span == len(SPANS) - 1
    begun = span > 0

    def kernel(*refs):
        parts, (a0, a1, w_ref), refs = refs[:8], refs[8:11], list(refs[11:])
        part_ref = refs.pop(0) if begun else None
        if begun:
            refs.pop(0)
        fg_ref, dg_ref, e_ref, x_ref, dg_tile, sems = refs
        y, xh, c, xl = (lax.axis_index(name) for name in ("y", "xh", "c", "xl"))

        def row(dy, dh, dc, j5):
            where = ((((y ^ dy) * 2 + (xh ^ dh)) * 2 + (c ^ dc)) * 2 + j5) * 32
            return pl.ds(pl.multiple_of(where, 32), 32)

        for flip in range(2):

            @pl.when(c == flip)
            def _(flip=flip):
                for dc in range(2):
                    for a in range(4):
                        for b in range(4):
                            dy, dx = (b, a) if flip ^ dc else (a, b)
                            e_ref[row(dy, dx >> 1, dc, xl ^ (dx & 1)), :] = parts[dc * 4 + a][
                                b * 32 : b * 32 + 32, :
                            ]

        for dh, act in enumerate((a0, a1)):
            for dc in range(2):
                for dy in range(4):
                    src = (dc * 4 + dy) * 64
                    where = (((y ^ dy) * 2 + (xh ^ dh)) * 2 + (c ^ dc)) * 64
                    x_ref[pl.ds(pl.multiple_of(where, 64), 64), :] = act[src : src + 64, :]
        error = e_ref[...]

        def out_copy(i):
            return pltpu.make_async_copy(
                dg_tile.at[i % 2],
                dg_ref.at[i * tile : (i + 1) * tile, begin:end],
                sems.at[i % 2],
            )

        for i in range(steps):
            cols = slice(i * tile, (i + 1) * tile)
            fg = lax.dot_general(
                error,
                w_ref[cols, begin:end],
                (((1,), (1,)), ((), ())),
                preferred_element_type=jnp.float32,
            )
            if begun:
                fg = fg + part_ref[:, cols]
            fg_ref[:, cols] = fg.astype(fg_ref.dtype)
            if i >= 2:
                out_copy(i - 2).wait()
            dg_tile[i % 2] = (
                lax.dot_general(
                    x_ref[:, cols],
                    error,
                    (((0,), (0,)), ((), ())),
                    preferred_element_type=jnp.float32,
                )
                * scale
            ).astype(jnp.bfloat16)
            out_copy(i).start()
        for i in range(steps - 2, steps):
            out_copy(i).wait()

    extra = [partial, made] if begun else []
    return pl.pallas_call(
        kernel,
        in_specs=[VMEM] * 11 + ([VMEM, HBM] if begun else []),
        out_specs=[VMEM, HBM],
        out_shape=[
            jax.ShapeDtypeStruct((tokens, feats), jnp.bfloat16 if last else jnp.float32),
            jax.ShapeDtypeStruct((feats, depth), jnp.bfloat16),
        ],
        input_output_aliases={12: 1} if begun else {},
        scratch_shapes=[
            pltpu.VMEM((tokens, width), jnp.bfloat16),
            pltpu.VMEM((tokens, feats), jnp.bfloat16),
            pltpu.VMEM((2, tile, width), jnp.bfloat16),
            pltpu.SemaphoreType.DMA((2,)),
        ],
        compiler_params=pltpu.CompilerParams(vmem_limit_bytes=32 * MIB),
        cost_estimate=pl.CostEstimate(
            flops=4 * tokens * feats * width,
            bytes_accessed=2 * (tokens * width + 2 * feats * width + 4 * tokens * feats),
            transcendentals=0,
        ),
        name="gradients",
    )(*mine, *theirs, *acts, decoder, *extra)


def body(sources, w_encode, b_encode, w_decode, b_decode, target):
    scale = 1.0 / math.sqrt(target.shape[0])
    block = sources[0]
    encoder, bias, decoder, own_block = prefetch(w_encode[0], b_encode, w_decode[0], block)

    across = move(block, by_xh)
    near = [own_block] + [move(block, by_y(k)) for k in (1, 2, 3)]
    far = [across, move(across, by_y(1)), move(near[2], by_xh), move(across, by_y(3))]

    near_acts = encode(near + [move(piece, by_core) for piece in near], encoder, bias)
    *far, near_acts = lax.optimization_barrier((*far, near_acts))
    keep_a, send_a, keep_b, send_b = decode(near_acts, decoder, SPANS)
    keeps, gots = [[keep_a], [keep_b]], [[move(send_a, by_core)], [move(send_b, by_core)]]
    far_acts = encode(far + [move(piece, by_core) for piece in far], encoder, bias)
    owns, firsts = [], []
    for span in range(len(SPANS)):
        keep, send = decode(far_acts, decoder, SPANS[span : span + 1])
        keeps[span].append(keep)
        gots[span].append(move(send, by_core))
    for span in range(len(SPANS)):
        own, *sends = split_cores(keeps[span], gots[span])
        owns.append(own)
        firsts.append([move(send, first(k + 1)) for k, send in enumerate(sends)])
    own, *sends = split_first(owns, firsts)
    own, low = add(own, [move(send, second(k + 1)) for k, send in enumerate(sends)])
    rows, low = finish(own, [move(low, by_z(k)) for k in (1, 2, 3)], target, b_decode[None])

    lows = join([low] + [move(low, second(k)) for k in (1, 2, 3)])
    feature_grad = decoder_grad = None
    acts = (near_acts, far_acts)
    for span, low in enumerate(lows):
        mine = [low] + [move(low, first(k)) for k in (1, 2, 3)]
        if span == len(lows) - 1:
            *mine, feature_grad = lax.optimization_barrier((*mine, feature_grad))
        theirs = [move(piece, by_core) for piece in mine]
        feature_grad, decoder_grad = gradients(
            mine, theirs, acts, decoder, scale, span, feature_grad, decoder_grad
        )
    rows = move(rows, owner)
    return rows, feature_grad[None], decoder_grad[None]


def solution(mesh):
    grid = Mesh(mesh.devices.reshape(2, 4, 4, 2, 2), AXES)
    return jax.shard_map(
        body,
        mesh=grid,
        in_specs=(
            P(LAYER, FEAT, None),
            P(LAYER, None, FEAT),
            P(LAYER, FEAT),
            P(LAYER, FEAT, None),
            P(),
            P(),
        ),
        out_specs=(P(AXES, None), P(LAYER, None, FEAT), P(LAYER, FEAT, None)),
        check_vma=False,
    )
```
